32 devices in a mesh: mp: 4 (over y, z), fsdp: 8 (over x, core).
Axes of the slice: x: 4, y: 2, z: 2, core: 2. Of those that a mesh axis runs over, the one named last changes fastest.
The devices are a block of a 4x4x8 slice.
Arguments:
- x: bfloat16 [2, 32, 2048, 768], P(None, ('mp', 'fsdp')), parts along dimension 1
- dy: bfloat16 [32, 2048, 768], P(('mp', 'fsdp')), parts along dimension 0
- xn: bfloat16 [32, 2048, 768], P(('mp', 'fsdp')), parts along dimension 0
- w1: float32 [2, 3072, 3072], P(None, ('mp', 'fsdp')), parts along dimension 1
- w2: float32 [2, 12288, 768], P(None, ('mp', 'fsdp')), parts along dimension 1
- g1: float32 [2, 3072, 3072], P(None, ('mp', 'fsdp')), parts along dimension 1
- g2: float32 [2, 12288, 768], P(None, ('mp', 'fsdp')), parts along dimension 1
- m1: float32 [2, 3072, 3072], P(None, ('mp', 'fsdp')), parts along dimension 1
- m2: float32 [2, 12288, 768], P(None, ('mp', 'fsdp')), parts along dimension 1
- v1: float32 [2, 3072, 3072], P(None, ('mp', 'fsdp')), parts along dimension 1
- v2: float32 [2, 12288, 768], P(None, ('mp', 'fsdp')), parts along dimension 1
- hp: float32 [5], replicated
- step: int32 [1], replicated
Outputs:
- output 1: float32 [2, 3072, 3072], P(None, ('mp', 'fsdp')), parts along dimension 1
- output 2: float32 [2, 12288, 768], P(None, ('mp', 'fsdp')), parts along dimension 1
- output 3: float32 [2, 3072, 3072], P(None, ('mp', 'fsdp')), parts along dimension 1
- output 4: float32 [2, 12288, 768], P(None, ('mp', 'fsdp')), parts along dimension 1
- output 5: float32 [2, 3072, 3072], P(None, ('mp', 'fsdp')), parts along dimension 1
- output 6: float32 [2, 12288, 768], P(None, ('mp', 'fsdp')), parts along dimension 1
- output 7: bfloat16 [32, 2048, 768], P(('mp', 'fsdp')), parts along dimension 0
There are 4 independent parts. The reference program is written for one: setup_inputs(seed, part) draws one part's arguments, and reference() takes and returns one part's arrays. A program takes and returns all parts, laid end to end along the dimension named above; an argument that names none is the same for every part.
All inputs are finite; a program needn't handle non-finite values.
Results may differ from the reference program's by a relative error of at most 0.00683772.
Values are sent between devices in bfloat16 or wider.
A program may use at most 768 MiB of HBM per device.

```python
import jax
import jax.numpy as jnp
from jax import lax

D = 768
FF = 3072
LAYERS = 2
BATCH_DEV = 1
SEQ = 2048
FSDP = 8


def gelu(h):
    return jax.nn.gelu(h, approximate=True)


def setup_inputs(seed: int = 0, part: int = 0) -> dict:
    kp = jax.random.fold_in(jax.random.key(seed), part)
    ks = jax.random.split(kp, 11)
    kc = jax.random.split(jax.random.key(seed + 1), 2)
    f32 = jnp.float32
    bf = jnp.bfloat16
    nb = FSDP * BATCH_DEV
    ntot = nb * SEQ
    u = jax.random.uniform(kc[0], (5,), f32)
    lr = (0.15 + 0.15 * u[0]) * D ** -0.5
    b1 = 0.85 + 0.07 * u[1]
    b2 = 0.95 + 0.04 * u[2]
    eps = 1e-8 * (1.0 + u[3])
    wd = 0.05 + 0.1 * u[4]
    hp = jnp.stack([lr, b1, b2, eps, wd]).astype(f32)
    step = jax.random.randint(kc[1], (1,), 2, 6, jnp.int32)
    tp = (step[0] - 1).astype(f32)
    c1 = 1.0 - b1 ** tp
    c2 = 1.0 - b2 ** tp
    gs1 = 0.35
    gs2 = 0.65
    s1 = (LAYERS, D, FF)
    s2 = (LAYERS, FF, D)
    return {
        'x': jax.random.normal(ks[0], (LAYERS, nb, SEQ, D), f32).astype(bf),
        'dy': (jax.random.normal(ks[1], (nb, SEQ, D), f32) * ntot ** -0.5).astype(bf),
        'xn': jax.random.normal(ks[2], (nb, SEQ, D), f32).astype(bf),
        'w1': jax.random.normal(ks[3], s1, f32) * D ** -0.5,
        'w2': jax.random.normal(ks[4], s2, f32) * FF ** -0.5,
        'g1': gs1 * jax.random.normal(ks[5], s1, f32),
        'g2': gs2 * jax.random.normal(ks[6], s2, f32),
        'm1': c1 * gs1 * jax.random.normal(ks[7], s1, f32),
        'm2': c1 * gs2 * jax.random.normal(ks[8], s2, f32),
        'v1': c2 * gs1 * gs1 * jax.random.uniform(ks[9], s1, f32, 0.5, 1.5),
        'v2': c2 * gs2 * gs2 * jax.random.uniform(ks[10], s2, f32, 0.5, 1.5),
        'hp': hp,
        'step': step,
    }


def reference(x, dy, xn, w1, w2, g1, g2, m1, m2, v1, v2, hp, step):
    f32 = jnp.float32
    bf = jnp.bfloat16
    nd = BATCH_DEV * SEQ
    wb1 = w1.astype(bf)
    wb2 = w2.astype(bf)
    xs = jnp.transpose(x.reshape(LAYERS, FSDP, nd, D), (1, 0, 2, 3))
    dys = dy.reshape(FSDP, nd, D)

    def one_device(carry, inp):
        xd, gy = inp
        acc1, acc2 = carry
        p1 = [None] * LAYERS
        p2 = [None] * LAYERS
        for l in reversed(range(LAYERS)):
            xl = xd[l]
            h = jnp.dot(xl, wb1[l], preferred_element_type=f32)
            a, gv = jax.vjp(gelu, h)
            a = a.astype(bf)
            da = jnp.dot(gy, wb2[l].T, preferred_element_type=f32)
            dh = gv(da)[0].astype(bf)
            p2[l] = jnp.dot(a.T, gy, preferred_element_type=f32).astype(bf)
            p1[l] = jnp.dot(xl.T, dh, preferred_element_type=f32).astype(bf)
            if l > 0:
                gy = (gy.astype(f32) + jnp.dot(dh, wb1[l].T, preferred_element_type=f32)).astype(bf)
        acc1 = acc1 + jnp.stack(p1).astype(f32)
        acc2 = acc2 + jnp.stack(p2).astype(f32)
        return (acc1, acc2), None

    init = (jnp.zeros((LAYERS, D, FF), f32), jnp.zeros((LAYERS, FF, D), f32))
    (s1, s2), _ = lax.scan(one_device, init, (xs, dys))
    tf = step[0].astype(f32)
    lr, b1, b2, eps, wd = hp[0], hp[1], hp[2], hp[3], hp[4]

    def adam(w, ga, s, m, v):
        g = (ga + s) / 2.0
        mn = b1 * m + (1.0 - b1) * g
        vn = b2 * v + (1.0 - b2) * g * g
        upd = (mn / (1.0 - b1 ** tf)) / (jnp.sqrt(vn / (1.0 - b2 ** tf)) + eps)
        return w - lr * (upd + wd * w), mn, vn

    nw1, nm1, nv1 = adam(w1, g1, s1, m1, v1)
    nw2, nm2, nv2 = adam(w2, g2, s2, m2, v2)
    nb1 = nw1.astype(bf)
    nb2 = nw2.astype(bf)

    def fwd(xc):
        for l in range(LAYERS):
            h = jnp.dot(xc, nb1[l], preferred_element_type=f32)
            a = gelu(h).astype(bf)
            xc = (xc.astype(f32) + jnp.dot(a, nb2[l], preferred_element_type=f32)).astype(bf)
        return xc

    xo = lax.map(fwd, xn.reshape(FSDP, nd, D)).reshape(FSDP * BATCH_DEV, SEQ, D)
    return (nw1, nw2, nm1, nm2, nv1, nv2, xo)
```

```python
import functools

import jax
import jax.numpy as jnp
from jax import lax
from jax.experimental import pallas as pl
from jax.experimental.pallas import tpu as pltpu
from jax.sharding import PartitionSpec as P

F32 = jnp.float32
BF = jnp.bfloat16
TM = 512
GC = 0.7978845608028654
GA = 0.044715


def gelu(h):
    return h * (0.5 * (1.0 + jnp.tanh(GC * (h + GA * (h * h * h)))))


def gelu_grad(h):
    s = h * h
    t = jnp.tanh(GC * (h + GA * (s * h)))
    cdf = 0.5 + 0.5 * t
    dt = (0.5 * GC) * (1.0 - t * t) * (1.0 + (3.0 * GA) * s)
    return h * cdf, cdf + h * dt


def dot(a, b):
    return jnp.dot(a, b, preferred_element_type=F32)


def dot_t(a, b):
    return lax.dot_general(a, b, (((1,), (1,)), ((), ())), preferred_element_type=F32)


def kernel(n, x, dy, xn, wb, w1, w2, g1, g2, m1, m2, v1, v2, sc,
           w1n, w2n, m1n, m2n, v1n, v2n, xo, go, gn, rp,
           xb, xt, yb, yt, ab, db, acc, p1, p2, pq, tb, ra, rb, nb, w1s, w2s,
           ag_s, ag_r, rs_s, rs_r, wsem, lsem, osem):
    nl, T, D = x.shape
    R = wb.shape[1]
    FB = 2 * R
    H = R // 2
    nc = n // 2
    D8 = D // n
    nt = T // TM
    me = lax.axis_index('fsdp')
    c = lax.div(me, 2)
    k = lax.rem(me, 2)
    cl, cr, co = lax.rem(c + nc - 1, nc), lax.rem(c + 1, nc), lax.rem(c + 2, nc)
    i, iq = 2 * c + k, 2 * c + 1 - k
    il, ir, io = 2 * cl + k, 2 * cr + k, 2 * co + k
    ilq, irq, ioq = 2 * cl + 1 - k, 2 * cr + 1 - k, 2 * co + 1 - k
    hA, hB = pl.ds(0, H), pl.ds(H, H)
    LEFT, RIGHT, MATE = il, ir, iq

    barrier = pltpu.get_barrier_semaphore()
    for dev in (LEFT, RIGHT, MATE):
        pl.semaphore_signal(barrier, inc=1, device_id={'fsdp': dev})
    pl.semaphore_wait(barrier, 3)

    pending = {}

    def rcopy(key, src, dst, ss, rs, dev):
        cp = pltpu.make_async_remote_copy(src_ref=src, dst_ref=dst, send_sem=ss, recv_sem=rs,
                                          device_id={'fsdp': dev})
        cp.start()
        pending[key] = cp

    def rwait(dst, ss, rs, dev):
        pltpu.make_async_remote_copy(src_ref=dst, dst_ref=dst, send_sem=ss, recv_sem=rs,
                                     device_id={'fsdp': dev}).wait_recv()

    def sent(key):
        cp = pending.pop(key, None)
        if cp is not None:
            cp.wait_send()

    class Gather:
        def __init__(self, ph, m, G, src):
            self.a, self.m, self.G, self.src = ph * 4 + m, m, G, src

        def put(self, t, src, dst, dev):
            rcopy(('ag', self.a, t), src, dst, ag_s.at[self.a, t], ag_r.at[self.a, t], dev)

        def got(self, t, dst, dev):
            rwait(dst, ag_s.at[self.a, t], ag_r.at[self.a, t], dev)

        def start(self):
            G, m, src = self.G, self.m, self.src
            self.put(0, src.at[hA], G.at[m, i, hA], RIGHT)
            self.put(3, src.at[hB], G.at[m, i, hB], LEFT)
            self.put(1, src.at[hB], G.at[m, i, hB], RIGHT)
            self.put(2, src.at[hA], G.at[m, i, hA], LEFT)
            self.put(4, src, G.at[m, i], MATE)

        def fwd(self):
            G, m = self.G, self.m
            self.got(0, G.at[m, il, hA], LEFT)
            self.put(5, G.at[m, il, hA], G.at[m, il, hA], RIGHT)
            self.got(3, G.at[m, ir, hB], RIGHT)
            self.put(6, G.at[m, ir, hB], G.at[m, ir, hB], LEFT)
            self.got(1, G.at[m, il, hB], LEFT)
            self.put(7, G.at[m, il], G.at[m, il], MATE)
            self.got(2, G.at[m, ir, hA], RIGHT)
            self.put(8, G.at[m, ir], G.at[m, ir], MATE)

        def fin(self):
            G, m = self.G, self.m
            self.got(5, G.at[m, io, hA], LEFT)
            self.got(6, G.at[m, io, hB], RIGHT)
            self.put(9, G.at[m, io], G.at[m, io], MATE)

        def mate(self, t):
            G, m = self.G, self.m
            j = {4: iq, 7: ilq, 8: irq, 9: ioq}[t]
            self.got(t, G.at[m, j], MATE)

        def full(self):
            for t in (4, 7, 8, 9):
                self.mate(t)

    old = [Gather(0, m, go, wb.at[m]) for m in range(2 * nl)]
    new = [Gather(1, m, gn, nb.at[m]) for m in range(2 * nl)]

    dest = (co, cr, cl, c)

    def rset(m):
        return 1 - m % 2

    def part(m):
        return p2 if m % 2 else p1

    def rput(m, t, src, dst, dev):
        rcopy(('rs', m, t), src, dst, rs_s.at[m, t], rs_r.at[m, t], dev)

    def rgot(m, t, dst, dev):
        rwait(dst, rs_s.at[m, t], rs_r.at[m, t], dev)

    def rs_x0(m, sl):
        rput(m, sl, part(m).at[2 * dest[sl] + 1 - k], pq.at[rset(m), sl], MATE)

    def rs_pair(m, sl):
        s = rset(m)
        for t in {0: (4, 5), 1: (6,), 2: (7,), 3: ()}[sl]:
            sent(('rs', m + 2, t))
        rgot(m, sl, pq.at[s, sl], MATE)
        sent(('rs', m, sl))
        tb[s, sl] = part(m)[2 * dest[sl] + k].astype(F32) + pq[s, sl].astype(F32)
        if sl == 0:
            rput(m, 4, tb.at[s, 0, hA], ra.at[m], LEFT)
            rput(m, 5, tb.at[s, 0, hB], rb.at[m], RIGHT)
        elif sl == 1:
            rput(m, 6, tb.at[s, 1, hA], rp.at[m, 0, hA], RIGHT)
        elif sl == 2:
            rput(m, 7, tb.at[s, 2, hB], rp.at[m, 1, hB], LEFT)

    def rs_mid(m):
        s = rset(m)
        rgot(m, 4, ra.at[m], RIGHT)
        ra[m] = ra[m] + tb[s, 2, hA]
        rput(m, 8, ra.at[m], rp.at[m, 1, hA], LEFT)
        rgot(m, 5, rb.at[m], LEFT)
        rb[m] = rb[m] + tb[s, 1, hB]
        rput(m, 9, rb.at[m], rp.at[m, 0, hB], RIGHT)

    def pieces(m, arr, row):
        l = m // 2
        if m % 2:
            return [(arr.at[l], acc.at[pl.ds(row, R)])]
        return [(arr.at[l, :, pl.ds(q * FB, FB)], acc.at[pl.ds(row + q * D8, D8)]) for q in range(nc)]

    ins = {0: (w1, g1, m1, v1), 1: (w2, g2, m2, v2)}
    outs = {0: (w1n, m1n, v1n), 1: (w2n, m2n, v2n)}

    def adam_copies(m):
        cps = []
        for j, arr in enumerate(ins[m % 2]):
            for hbm, vm in pieces(m, arr, j * R):
                cps.append(pltpu.make_async_copy(hbm, vm, lsem.at[len(cps)]))
        return cps

    def adam_load(m):
        for cp in adam_copies(m):
            cp.start()

    def adam_outs(m):
        cps = []
        for arr, row in zip(outs[m % 2], (0, 2 * R, 3 * R)):
            for hbm, vm in pieces(m, arr, row):
                cps.append(pltpu.make_async_copy(vm, hbm, osem.at[len(cps)]))
        return cps

    def adam_run(m):
        s = rset(m)
        for t, dst, dev in ((6, rp.at[m, 0, hA], LEFT), (9, rp.at[m, 0, hB], LEFT),
                            (8, rp.at[m, 1, hA], RIGHT), (7, rp.at[m, 1, hB], RIGHT)):
            rgot(m, t, dst, dev)
        cps = [pltpu.make_async_copy(rp.at[m, e], acc.at[pl.ds((4 + e) * R, R)], lsem.at[16 + e])
               for e in range(2)]
        for cp in cps:
            cp.start()
        for cp in adam_copies(m) + cps:
            cp.wait()
        lr, b1, b2, eps, wd, c1, c2 = [sc[j] for j in range(7)]
        ch = 32

        @pl.loop(0, R // ch)
        def _(e):
            o = pl.multiple_of(e * ch, ch)
            rows = [pl.ds(j * R + o, ch) for j in range(6)]
            S = tb[s, 3, pl.ds(o, ch)] + acc[rows[4]] + acc[rows[5]]
            w = acc[rows[0]]
            g = (acc[rows[1]] + S) * 0.5
            mn = b1 * acc[rows[2]] + (1.0 - b1) * g
            vn = b2 * acc[rows[3]] + (1.0 - b2) * g * g
            upd = (mn / c1) / (jnp.sqrt(vn / c2) + eps)
            wn = w - lr * (upd + wd * w)
            acc[rows[0]] = wn
            acc[rows[2]] = mn
            acc[rows[3]] = vn
            nb[m, pl.ds(o, ch)] = wn.astype(BF)

        for cp in adam_outs(m):
            cp.start()

    def adam_done(m):
        for cp in adam_outs(m):
            cp.wait()

    def wcopies(G, l, q, slot):
        return (pltpu.make_async_copy(G.at[2 * l, :, pl.ds(q * D8, D8)], w1s.at[slot], wsem.at[slot, 0]),
                pltpu.make_async_copy(G.at[2 * l + 1, pl.ds(2 * q, 2)], w2s.at[slot], wsem.at[slot, 1]))

    def wload(*a):
        for cp in wcopies(*a):
            cp.start()

    def wwait(*a):
        for cp in wcopies(*a):
            cp.wait()

    def tile(t):
        return pl.ds(pl.multiple_of(t * TM, TM), TM)

    def w1v(slot):
        return w1s[slot].reshape(D, FB)

    def w2v(slot):
        return w2s[slot].reshape(FB, D)

    def bwd_fused(slot):
        @pl.loop(0, nt)
        def _(t):
            r = tile(t)
            h = dot(xb[r, :], w1v(slot))
            da = dot_t(yb[r, :], w2v(slot))
            a, gp = gelu_grad(h)
            ab[r, :] = a.astype(BF)
            db[r, :] = (da * gp).astype(BF)

    def bwd_p2(q):
        @pl.loop(0, D // 256)
        def _(t):
            o = pl.ds(pl.multiple_of(t * 256, 256), 256)
            r = dot(yt[o, :], ab[...])
            p2[pl.ds(2 * q, 2), :, o] = r.T.astype(BF).reshape(2, R, 256)

    def bwd_p1(q):
        @pl.loop(0, 2)
        def _(t):
            o = pl.ds(pl.multiple_of(t * (D // 2), D // 2), D // 2)
            r = dot(xt[o, :], db[...])
            p1[pl.ds(t * (n // 2), n // 2), pl.ds(pl.multiple_of(q * D8, D8), D8), :] = (
                r.astype(BF).reshape(n // 2, D8, FB))

    def bwd_dx(slot, first):
        @pl.loop(0, nt)
        def _(t):
            r = tile(t)
            z = dot_t(db[r, :], w1v(slot))
            acc[r, :] = z if first else acc[r, :] + z

    def transpose(dst, src):
        @pl.loop(0, T // 256)
        def _(t):
            o = pl.ds(pl.multiple_of(t * 256, 256), 256)
            dst[:, o] = src[o, :].T

    def fwd_block(slot, first, last):
        @pl.loop(0, nt)
        def _(t):
            r = tile(t)
            a = gelu(dot(xb[r, :], w1v(slot))).astype(BF)
            z = dot(a, w2v(slot))
            if not first:
                z = acc[r, :] + z
            if last:
                xb[r, :] = (xb[r, :].astype(F32) + z).astype(BF)
            else:
                acc[r, :] = z

    old[2].start()
    old[3].start()
    own_in = [pltpu.make_async_copy(wb, nb, lsem.at[0]),
              pltpu.make_async_copy(x.at[1], xb, lsem.at[1]),
              pltpu.make_async_copy(dy, yb, lsem.at[2])]
    for cp in own_in:
        cp.start()
    own_in[0].wait()
    own_out = [pltpu.make_async_copy(nb.at[m], go.at[m, i], osem.at[m]) for m in range(2 * nl)]
    for cp in own_out:
        cp.start()
    own_in[1].wait()
    own_in[2].wait()
    old[2].fwd()
    transpose(xt, xb)
    for cp in own_out:
        cp.wait()
    old[3].fwd()
    old[0].start()
    old[1].start()
    transpose(yt, yb)
    old[2].fin()
    old[2].full()
    old[3].fin()
    old[3].full()

    wload(go, 1, dest[0], 0)
    for j in range(nc):
        q, s = dest[j], j % 2
        if j + 1 < nc:
            wload(go, 1, dest[j + 1], 1 - s)
        wwait(go, 1, q, s)
        bwd_fused(s)
        if j == 3:
            rs_pair(3, 1)
        bwd_p2(q)
        rs_x0(3, j)
        if j in (1, 2):
            rs_pair(3, j - 1) if j == 1 else None
        bwd_p1(q)
        if j == 0:
            old[0].fwd()
        elif j == 1:
            old[1].fwd()
        elif j == 2:
            old[0].fin()
        else:
            old[1].fin()
            rs_pair(3, 2)
            for sl in range(4):
                rs_x0(2, sl)
        bwd_dx(s, j == 0)
    xin = pltpu.make_async_copy(x.at[0], xb, lsem.at[0])
    xin.start()
    rs_mid(3)
    rs_pair(3, 3)
    for sl in range(4):
        rs_pair(2, sl)

    @pl.loop(0, nt)
    def _(t):
        r = tile(t)
        yb[r, :] = (yb[r, :].astype(F32) + acc[r, :]).astype(BF)

    transpose(yt, yb)
    xin.wait()
    transpose(xt, xb)
    old[0].full()
    old[1].full()

    adam_load(3)
    wload(go, 0, dest[0], 0)
    for j in range(nc):
        q, s = dest[j], j % 2
        if j + 1 < nc:
            wload(go, 0, dest[j + 1], 1 - s)
        wwait(go, 0, q, s)
        bwd_fused(s)
        if j == 1:
            rs_mid(2)
        if j == 2:
            rs_pair(1, 1)
        if j == 3:
            rs_pair(1, 2)
        bwd_p2(q)
        rs_x0(1, j)
        bwd_p1(q)
        if j == 1:
            rs_pair(1, 0)
            adam_run(3)
    for sl in range(4):
        rs_x0(0, sl)
    adam_done(3)
    adam_load(2)
    xin = pltpu.make_async_copy(xn, xb, wsem.at[0, 0])
    xin.start()
    rs_mid(1)
    rs_pair(1, 3)
    adam_run(2)
    for sl in range(4):
        rs_pair(0, sl)
    adam_done(2)
    adam_load(1)
    rs_mid(0)
    adam_run(1)
    new[1].start()
    adam_done(1)
    adam_load(0)
    new[1].fwd()
    adam_run(0)
    new[0].start()
    adam_done(0)
    new[0].fwd()
    new[2].start()
    new[3].start()
    new[1].fin()
    new[1].full()
    xin.wait()
    own_out = [pltpu.make_async_copy(nb.at[m], gn.at[m, i], osem.at[m]) for m in range(2 * nl)]
    for cp in own_out:
        cp.start()
    for cp in own_out:
        cp.wait()
    new[0].fin()
    new[0].full()

    order = (c, cr, cl, co)
    wload(gn, 0, order[0], 0)
    for j in range(nc):
        s = j % 2
        if j + 1 < nc:
            wload(gn, 0, order[j + 1], 1 - s)
        wwait(gn, 0, order[j], s)
        fwd_block(s, j == 0, j == nc - 1)
        if j == 0:
            new[2].fwd()
        elif j == 1:
            new[3].fwd()
        elif j == 2:
            new[2].fin()
    new[2].full()
    new[3].mate(4)
    wload(gn, 1, order[0], 0)
    for j in range(nc):
        s = j % 2
        if j == 0:
            new[3].mate(8)
        elif j == 1:
            new[3].mate(7)
        elif j == 2:
            new[3].fin()
            new[3].mate(9)
        if j + 1 < nc:
            wload(gn, 1, order[j + 1], 1 - s)
        wwait(gn, 1, order[j], s)
        fwd_block(s, j == 0, j == nc - 1)
    out = pltpu.make_async_copy(xb, xo, lsem.at[0])
    out.start()
    out.wait()
    for key in list(pending):
        sent(key)


def solution(mesh):
    n = mesh.shape['fsdp']
    tok4 = P(None, ('mp', 'fsdp'), None, None)
    tok3 = P(('mp', 'fsdp'), None, None)
    rows = P(None, ('mp', 'fsdp'), None)

    def body(x, dy, xn, w1, w2, g1, g2, m1, m2, v1, v2, hp, step):
        nl, b, t, d = x.shape
        T = b * t
        R = w2.shape[1]
        FB = 2 * R
        nc = n // 2
        tf = step[0].astype(F32)
        sc = jnp.concatenate([hp, (1.0 - hp[1] ** tf)[None], (1.0 - hp[2] ** tf)[None]])
        b1 = w1.astype(BF).reshape(nl, d // n, nc, FB).transpose(0, 2, 1, 3).reshape(nl, 1, R, d)
        wb = jnp.concatenate([b1, w2.astype(BF).reshape(nl, 1, R, d)], axis=1).reshape(2 * nl, R, d)
        hbm = pl.BlockSpec(memory_space=pltpu.HBM)
        sd = jax.ShapeDtypeStruct
        res = pl.pallas_call(
            functools.partial(kernel, n),
            out_shape=[sd(w1.shape, F32), sd(w2.shape, F32)] * 3 + [
                sd((T, d), BF), sd((2 * nl, n, R, d), BF), sd((2 * nl, n, R, d), BF),
                sd((2 * nl, 2, R, d), F32)],
            in_specs=[hbm] * 12 + [pl.BlockSpec(memory_space=pltpu.SMEM)],
            out_specs=[hbm] * 10,
            scratch_shapes=[
                pltpu.VMEM((T, d), BF), pltpu.VMEM((d, T), BF),
                pltpu.VMEM((T, d), BF), pltpu.VMEM((d, T), BF),
                pltpu.VMEM((T, FB), BF), pltpu.VMEM((T, FB), BF),
                pltpu.VMEM((max(6 * R, T), d), F32),
                pltpu.VMEM((n, R, d), BF), pltpu.VMEM((n, R, d), BF),
                pltpu.VMEM((2, nc, R, d), BF),
                pltpu.VMEM((2, nc, R, d), F32),
                pltpu.VMEM((2 * nl, R // 2, d), F32), pltpu.VMEM((2 * nl, R // 2, d), F32),
                pltpu.VMEM((2 * nl, R, d), BF),
                pltpu.VMEM((2, n, d // n, FB), BF), pltpu.VMEM((2, 2, R, d), BF),
                pltpu.SemaphoreType.DMA((4 * nl, 10)), pltpu.SemaphoreType.DMA((4 * nl, 10)),
                pltpu.SemaphoreType.DMA((2 * nl, 10)), pltpu.SemaphoreType.DMA((2 * nl, 10)),
                pltpu.SemaphoreType.DMA((2, 2)), pltpu.SemaphoreType.DMA((18,)),
                pltpu.SemaphoreType.DMA((12,)),
            ],
            compiler_params=pltpu.CompilerParams(
                collective_id=0, has_side_effects=True, vmem_limit_bytes=67043328),
        )(x.reshape(nl, T, d), dy.reshape(T, d), xn.reshape(T, d), wb,
          w1, w2, g1, g2, m1, m2, v1, v2, sc)
        return tuple(res[:6]) + (res[6].reshape(b, t, d),)

    return jax.shard_map(body, mesh=mesh,
                         in_specs=(tok4, tok3, tok3) + (rows,) * 8 + (P(), P()),
                         out_specs=(rows,) * 6 + (tok3,), check_vma=False)
```

```python
import functools

import jax
import jax.numpy as jnp
from jax import lax
from jax.experimental import pallas as pl
from jax.experimental.pallas import tpu as pltpu
from jax.sharding import PartitionSpec as P

F32 = jnp.float32
BF = jnp.bfloat16
TM = 512
TF = 1024
GC = 0.7978845608028654
GA = 0.044715


def gelu(h):
    return h * (0.5 * (1.0 + jnp.tanh(GC * (h + GA * (h * h * h)))))


def gelu_grad(h):
    s = h * h
    t = jnp.tanh(GC * (h + GA * (s * h)))
    cdf = 0.5 + 0.5 * t
    dt = (0.5 * GC) * (1.0 - t * t) * (1.0 + (3.0 * GA) * s)
    return h * cdf, cdf + h * dt


def dot(a, b):
    return jnp.dot(a, b, preferred_element_type=F32)


def dot_t(a, b):
    return lax.dot_general(a, b, (((1,), (1,)), ((), ())), preferred_element_type=F32)


def offset(j):
    if isinstance(j, int):
        return (2, 1, 3, 0)[j]
    return jnp.where(j == 0, 2, jnp.where(j == 1, 1, jnp.where(j == 2, 3, 0)))


def ipow(b, t):
    r = b * b
    for e in (3, 4, 5):
        r = r * jnp.where(t >= e, b, 1.0)
    return r


def kernel(n, x, dy, xn, w1, w2, g1, g2, m1, m2, v1, v2, hp, step,
           w1n, w2n, m1n, m2n, v1n, v2n, zo, go, gn, rp,
           xb, xt, yb, yt, ab, db, acc, p1, p2, pq, tb, ra, rb, nb, w1s, w2s,
           ag_s, ag_r, rs_s, rs_r, wsem, lsem, osem):
    nl, T, D = x.shape
    R = w2.shape[1]
    FB = 2 * R
    H = R // 2
    nc = n // 2
    D8 = D // n
    nt = T // TM
    me = lax.axis_index('fsdp')
    c = lax.div(me, 2)
    k = lax.rem(me, 2)
    cl, cr, co = lax.rem(c + nc - 1, nc), lax.rem(c + 1, nc), lax.rem(c + 2, nc)
    i, iq = 2 * c + k, 2 * c + 1 - k
    il, ir, io = 2 * cl + k, 2 * cr + k, 2 * co + k
    ilq, irq, ioq = 2 * cl + 1 - k, 2 * cr + 1 - k, 2 * co + 1 - k
    hA, hB = pl.ds(0, H), pl.ds(H, H)
    LEFT, RIGHT, MATE = il, ir, iq

    barrier = pltpu.get_barrier_semaphore()
    for dev in (LEFT, RIGHT, MATE):
        pl.semaphore_signal(barrier, inc=1, device_id={'fsdp': dev})

    pending = {}

    def rmake(src, dst, ss, rs, dev):
        return pltpu.make_async_remote_copy(
            src_ref=src[0].at[src[1:]], dst_ref=dst[0].at[dst[1:]], send_sem=ss[0].at[ss[1:]],
            recv_sem=rs[0].at[rs[1:]], device_id={'fsdp': dev})

    def rcopy(key, *a):
        rmake(*a).start()
        pending[key] = a

    def rwait(dst, ss, rs, dev):
        rmake(dst, dst, ss, rs, dev).wait_recv()

    def sent(key):
        a = pending.pop(key, None)
        if a is not None:
            rmake(*a).wait_send()

    class Gather:
        def __init__(self, ph, m, G, src):
            self.a, self.m, self.G, self.src = ph * 4 + m, m, G, src

        def put(self, t, src, dst, dev):
            rcopy(('ag', self.a, t), src, dst, (ag_s, self.a, t), (ag_r, self.a, t), dev)

        def got(self, t, dst, dev):
            rwait(dst, (ag_s, self.a, t), (ag_r, self.a, t), dev)

        def start(self):
            self.start_a()
            self.start_b()

        def fwd(self):
            self.fwd_a()
            self.fwd_b()

        def start_a(self):
            G, m, src = self.G, self.m, self.src
            self.put(0, src + (hA,), (G, m, i, hA), RIGHT)
            self.put(3, src + (hB,), (G, m, i, hB), LEFT)
            self.put(4, src, (G, m, i), MATE)

        def start_b(self):
            G, m, src = self.G, self.m, self.src
            self.put(1, src + (hB,), (G, m, i, hB), RIGHT)
            self.put(2, src + (hA,), (G, m, i, hA), LEFT)

        def fwd_a(self):
            G, m = self.G, self.m
            self.got(0, (G, m, il, hA), LEFT)
            self.put(5, (G, m, il, hA), (G, m, il, hA), RIGHT)
            self.got(3, (G, m, ir, hB), RIGHT)
            self.put(6, (G, m, ir, hB), (G, m, ir, hB), LEFT)

        def fwd_b(self):
            G, m = self.G, self.m
            self.got(1, (G, m, il, hB), LEFT)
            self.put(7, (G, m, il), (G, m, il), MATE)
            self.got(2, (G, m, ir, hA), RIGHT)
            self.put(8, (G, m, ir), (G, m, ir), MATE)

        def fin(self):
            G, m = self.G, self.m
            self.got(5, (G, m, io, hA), LEFT)
            self.got(6, (G, m, io, hB), RIGHT)
            self.put(9, (G, m, io), (G, m, io), MATE)

        def mate(self, t):
            G, m = self.G, self.m
            j = {4: iq, 7: ilq, 8: irq, 9: ioq}[t]
            self.got(t, (G, m, j), MATE)

        def full(self):
            for t in (4, 7, 8, 9):
                self.mate(t)

    old = [Gather(0, m, go, (nb, m)) for m in range(2 * nl)]
    new = [Gather(1, m, gn, (nb, m)) for m in range(2 * nl)]

    dest = (co, cr, cl, c)
    mine = tuple(2 * d + k for d in dest)
    theirs = tuple(2 * d + 1 - k for d in dest)

    def rset(m):
        return 1 - m % 2

    def part(m):
        return p2 if m % 2 else p1

    def rput(m, t, src, dst, dev):
        rcopy(('rs', m, t), src, dst, (rs_s, m, t), (rs_r, m, t), dev)

    def rgot(m, t, dst, dev):
        rwait(dst, (rs_s, m, t), (rs_r, m, t), dev)

    def x0_copy(m, sl):
        return rmake((part(m), theirs[sl]), (pq, rset(m), sl), (rs_s, m, sl), (rs_r, m, sl), MATE)

    def rs_x0(m, sl):
        x0_copy(m, sl).start()

    def rs_pair(m, sl):
        s = rset(m)
        for t in {0: (4, 5), 1: (6,), 2: (7,), 3: ()}[sl]:
            sent(('rs', m + 2, t))
        rgot(m, sl, (pq, s, sl), MATE)
        x0_copy(m, sl).wait_send()
        tb[s, sl] = part(m)[mine[sl]].astype(F32) + pq[s, sl].astype(F32)
        if sl == 0:
            rput(m, 4, (tb, s, 0, hA), (ra, m), LEFT)
            rput(m, 5, (tb, s, 0, hB), (rb, m), RIGHT)
        elif sl == 1:
            rput(m, 6, (tb, s, 1, hA), (rp, m, 0, hA), RIGHT)
        elif sl == 2:
            rput(m, 7, (tb, s, 2, hB), (rp, m, 1, hB), LEFT)

    def rs_mid(m):
        s = rset(m)
        rgot(m, 4, (ra, m), RIGHT)
        ra[m] = ra[m] + tb[s, 2, hA]
        rput(m, 8, (ra, m), (rp, m, 1, hA), LEFT)
        rgot(m, 5, (rb, m), LEFT)
        rb[m] = rb[m] + tb[s, 1, hB]
        rput(m, 9, (rb, m), (rp, m, 0, hB), RIGHT)

    def pieces(m, arr, row):
        l = m // 2
        if m % 2:
            return [(arr.at[l], acc.at[pl.ds(row, R)])]
        return [(arr.at[l, :, pl.ds(q * FB, FB)], acc.at[pl.ds(row + q * D8, D8)]) for q in range(nc)]

    ins = {0: (w1, g1, m1, v1), 1: (w2, g2, m2, v2)}
    outs = {0: (w1n, m1n, v1n), 1: (w2n, m2n, v2n)}

    def adam_copies(m):
        cps = []
        for j, arr in enumerate(ins[m % 2]):
            for hbm, vm in pieces(m, arr, j * R):
                cps.append(pltpu.make_async_copy(hbm, vm, lsem.at[len(cps)]))
        return cps

    def adam_load(m):
        for cp in adam_copies(m):
            cp.start()

    def adam_outs(m):
        cps = []
        for arr, row in zip(outs[m % 2], (0, 2 * R, 3 * R)):
            for hbm, vm in pieces(m, arr, row):
                cps.append(pltpu.make_async_copy(vm, hbm, osem.at[len(cps)]))
        return cps

    def adam_run(m):
        s = rset(m)
        for t, dst, dev in ((6, (rp, m, 0, hA), LEFT), (9, (rp, m, 0, hB), LEFT),
                            (8, (rp, m, 1, hA), RIGHT), (7, (rp, m, 1, hB), RIGHT)):
            rgot(m, t, dst, dev)
        cps = [pltpu.make_async_copy(rp.at[m, e], acc.at[pl.ds((4 + e) * R, R)], lsem.at[16 + e])
               for e in range(2)]
        for cp in cps:
            cp.start()
        for cp in adam_copies(m) + cps:
            cp.wait()
        for t in range(5):
            sent(('ag', m, t))
        lr, b1, b2, eps, wd = [hp[j] for j in range(5)]
        c1 = 1.0 - ipow(b1, step[0])
        c2 = 1.0 - ipow(b2, step[0])
        ch = 32

        @pl.loop(0, R // ch)
        def _(e):
            o = pl.multiple_of(e * ch, ch)
            rows = [pl.ds(j * R + o, ch) for j in range(6)]
            S = tb[s, 3, pl.ds(o, ch)] + acc[rows[4]] + acc[rows[5]]
            w = acc[rows[0]]
            g = (acc[rows[1]] + S) * 0.5
            mn = b1 * acc[rows[2]] + (1.0 - b1) * g
            vn = b2 * acc[rows[3]] + (1.0 - b2) * g * g
            upd = (mn / c1) / (jnp.sqrt(vn / c2) + eps)
            wn = w - lr * (upd + wd * w)
            acc[rows[0]] = wn
            acc[rows[2]] = mn
            acc[rows[3]] = vn
            nb[m, pl.ds(o, ch)] = wn.astype(BF)

        for cp in adam_outs(m):
            cp.start()

    def adam_done(m):
        for cp in adam_outs(m):
            cp.wait()

    def wcopy(G, l, q, slot, kind):
        if kind:
            return pltpu.make_async_copy(G.at[2 * l + 1, pl.ds(2 * q, 2)], w2s.at[slot], wsem.at[slot, 1])
        return pltpu.make_async_copy(G.at[2 * l, :, pl.ds(q * D8, D8)], w1s.at[slot], wsem.at[slot, 0])

    def wcopies(*a):
        return wcopy(*a, 0), wcopy(*a, 1)

    def wload(*a):
        for cp in wcopies(*a):
            cp.start()

    def wwait(*a):
        for cp in wcopies(*a):
            cp.wait()

    def tile(t):
        return pl.ds(pl.multiple_of(t * TM, TM), TM)

    def w1v(slot):
        return w1s[slot].reshape(D, FB)

    def w2v(slot):
        return w2s[slot].reshape(FB, D)

    def bwd_fused(slot):
        @pl.loop(0, nt)
        def _(t):
            r = tile(t)
            h = dot(xb[r, :], w1v(slot))
            da = dot_t(yb[r, :], w2v(slot))
            a, gp = gelu_grad(h)
            ab[r, :] = a.astype(BF)
            db[r, :] = (da * gp).astype(BF)

    def bwd_p2(q):
        @pl.loop(0, D // 256)
        def _(t):
            o = pl.ds(pl.multiple_of(t * 256, 256), 256)
            r = dot(yt[o, :], ab[...])
            p2[pl.ds(2 * q, 2), :, o] = r.T.astype(BF).reshape(2, R, 256)

    def bwd_p1(q):
        @pl.loop(0, 2)
        def _(t):
            o = pl.ds(pl.multiple_of(t * (D // 2), D // 2), D // 2)
            r = dot(xt[o, :], db[...])
            p1[pl.ds(t * (n // 2), n // 2), pl.ds(pl.multiple_of(q * D8, D8), D8), :] = (
                r.astype(BF).reshape(n // 2, D8, FB))

    def bwd_dx(slot, first):
        @pl.loop(0, nt)
        def _(t):
            r = tile(t)
            z = dot_t(db[r, :], w1v(slot))
            acc[r, :] = jnp.where(first, yb[r, :].astype(F32), acc[r, :]) + z

    def transpose(dst, src):
        @pl.loop(0, T // 256)
        def _(t):
            o = pl.ds(pl.multiple_of(t * 256, 256), 256)
            dst[:, o] = src[o, :].T

    order = (c, cr, cl, co)
    abuf = (ab, db, yb, xb)

    def hidden(l, hooks):
        cps = [wcopy(gn, l, order[j], j % 2, 0) for j in range(nc)]
        cps[0].start()
        for j in range(nc):
            if j + 1 < nc:
                cps[j + 1].start()
            cps[j].wait()

            @pl.loop(0, nt)
            def _(t):
                r = tile(t)
                xv = xb[r, :]
                if j == 0:
                    acc[r, :] = xv.astype(F32)
                abuf[j][r, :] = gelu(dot(xv, w1v(j % 2))).astype(BF)
            if j in hooks:
                with jax.named_scope(f'hookH{j}'):
                    hooks[j]()

    def project(l, ready, hooks, done, late):
        cps = [wcopy(gn, l, order[j], j % 2, 1) for j in range(nc)]
        ready(0)
        cps[0].start()
        for j in range(nc):
            if j + 1 < late:
                with jax.named_scope(f'ready{j + 1}'):
                    ready(j + 1)
                cps[j + 1].start()
            elif j >= late:
                with jax.named_scope(f'ready{j}'):
                    ready(j)
                cps[j].start()
            cps[j].wait()

            @pl.loop(0, nt)
            def _(t):
                r = tile(t)
                z = acc[r, :] + dot(abuf[j][r, :], w2v(j % 2))
                if j == nc - 1:
                    xb[r, :] = z.astype(BF)
                    done(t)
                else:
                    acc[r, :] = z
            if j in hooks:
                with jax.named_scope(f'hookP{j}'):
                    hooks[j]()

    def narrow(dst):
        @pl.loop(0, nt)
        def _(t):
            r = tile(t)
            dst[r, :] = acc[r, :].astype(BF)

    def at(j, hooks):
        for jj, fn in hooks.items():
            @pl.when(j == jj)
            def _():
                fn()

    def blocks(G, l, off, count, stages, ready=None):
        wload(G, l, lax.rem(c + off(0), nc), 0)

        @pl.loop(0, count)
        def _(j):
            s = lax.rem(j, 2)
            q = lax.rem(c + off(j), nc)

            @pl.when(j + 1 < count)
            def _():
                wload(G, l, lax.rem(c + off(j + 1), nc), 1 - s)
            wwait(G, l, q, s)
            for name, fn, hooks in stages:
                with jax.named_scope(name):
                    fn(j, q, s)
                with jax.named_scope(name + 'Hook'):
                    at(j, hooks)

    scope = jax.named_scope

    with scope('start'):
        w_in = [[pltpu.make_async_copy(a, b, lsem.at[m * 4 + e])
                 for e, (a, b) in enumerate(pieces(m, ins[m % 2][0], m * R))] for m in range(2 * nl)]
        for m in (2, 3, 0, 1):
            for cp in w_in[m]:
                cp.start()
        tok_in = [pltpu.make_async_copy(x.at[1], xb, wsem.at[0, 0]),
                  pltpu.make_async_copy(dy, yb, wsem.at[0, 1])]
        for cp in tok_in:
            cp.start()
        own_out = [pltpu.make_async_copy(nb.at[m], go.at[m, i], osem.at[m]) for m in range(2 * nl)]
        for m in (2, 3, 0, 1):
            for cp in w_in[m]:
                cp.wait()
            nb[m] = acc[pl.ds(m * R, R), :].astype(BF)
            if m == 2:
                pl.semaphore_wait(barrier, 3)
            if m >= 2:
                old[m].start()
            own_out[m].start()
        for cp in tok_in:
            cp.wait()
    with scope('f2'):
        old[2].fwd()
    with scope('xt'):
        transpose(xt, xb)
        for cp in own_out:
            cp.wait()
    with scope('f3'):
        old[3].fwd()
        old[0].start()
        old[1].start()
    with scope('yt'):
        transpose(yt, yb)
    with scope('full23'):
        old[2].fin()
        old[2].full()
        old[3].fin()
        old[3].full()

    def c2_2():
        old[0].fin()
        rs_pair(3, 2)

    def c2_3():
        old[1].fin()
        for sl in range(4):
            rs_x0(2, sl)
        rs_pair(3, 3)

    blocks(go, 1, offset, nc, [
        ('A2', lambda j, q, s: bwd_fused(s), {2: lambda: rs_pair(3, 1), 3: lambda: rs_mid(3)}),
        ('B2', lambda j, q, s: bwd_p2(q), {
            0: lambda: rs_x0(3, 0),
            1: lambda: (rs_x0(3, 1), rs_pair(3, 0)),
            2: lambda: rs_x0(3, 2),
            3: lambda: rs_x0(3, 3)}),
        ('C2', lambda j, q, s: bwd_p1(q), {
            0: old[0].fwd, 1: old[1].fwd, 2: c2_2, 3: c2_3}),
        ('D2', lambda j, q, s: bwd_dx(s, j == 0), {}),
    ])
    with scope('mid2'):
        xin = pltpu.make_async_copy(x.at[0], xb, lsem.at[0])
        xin.start()
        for sl in range(4):
            rs_pair(2, sl)
    with scope('tr2'):
        narrow(yb)
        transpose(yt, yb)
        xin.wait()
        transpose(xt, xb)
    with scope('full01'):
        old[0].full()
        old[1].full()

    adam_load(3)

    def up3():
        rs_pair(1, 0)
        adam_run(3)

    def up2():
        adam_done(3)
        adam_load(2)

    def up1():
        rs_pair(1, 2)
        adam_run(2)

    blocks(go, 0, offset, nc, [
        ('A1', lambda j, q, s: bwd_fused(s), {
            1: lambda: rs_mid(2), 2: lambda: rs_pair(1, 1), 3: up1}),
        ('B1', lambda j, q, s: bwd_p2(q), {jj: functools.partial(rs_x0, 1, jj) for jj in range(nc)}),
        ('C1', lambda j, q, s: bwd_p1(q), {1: up3, 2: up2}),
    ])
    with scope('mid1'):
        for sl in range(4):
            rs_x0(0, sl)
        xin = pltpu.make_async_copy(xn, xb, wsem.at[0, 0])
        xin.start()
        adam_done(2)
        adam_load(1)
        rs_mid(1)
        rs_pair(1, 3)
        for sl in range(4):
            rs_pair(0, sl)
    with scope('adam1'):
        adam_run(1)
        adam_done(1)
        adam_load(0)
    with scope('mid0'):
        rs_mid(0)
        new[1].start_a()
    own_out = [pltpu.make_async_copy(nb.at[m], gn.at[m, i], wsem.at[m // 2, m % 2]) for m in range(2 * nl)]
    with scope('adam0'):
        xin.wait()
        adam_run(0)
        new[0].start()
        for cp in own_out:
            cp.start()
    with scope('fn0'):
        new[0].fwd_a()
        new[1].start_b()
        new[1].fwd_a()
        new[0].fwd_b()
        for cp in own_out:
            cp.wait()
        adam_done(0)
    with scope('full_n0'):
        new[0].fin()
        new[2].start()
        new[0].full()

    def nx2():
        new[2].fwd_a()
        new[3].start()

    with scope('H1'):
        hidden(0, {1: new[1].fwd_b, 3: new[1].fin})
    with scope('P1'):
        project(0, lambda j: new[1].mate((4, 8, 7, 9)[j]), {0: nx2, 2: new[2].fwd_b}, lambda t: None, nc)
    with scope('full_n2'):
        new[2].fin()
        new[2].full()

    w1c = [wcopy(gn, 1, order[j], j % 2, 0) for j in range(nc)]
    w2c = [wcopy(gn, 1, order[j], j % 2, 1) for j in range(nc)]

    def step(hj=None, pj=None, last=False, hook=None):
        @pl.loop(0, T // TF)
        def _(t):
            r = pl.ds(pl.multiple_of(t * TF, TF), TF)
            if hook is not None:
                @pl.when(t == T // TF - 1)
                def _():
                    hook()
            if pj is not None:
                z = acc[r, :] + dot(abuf[pj][r, :], w2v(pj % 2))
            if hj is not None:
                xv = xb[r, :]
                if hj == 0:
                    acc[r, :] = xv.astype(F32)
                abuf[hj][r, :] = gelu(dot(xv, w1v(hj % 2))).astype(BF)
            if last:
                xb[r, :] = z.astype(BF)
                zout(t).start()
            elif pj is not None:
                acc[r, :] = z

    def zout(t):
        r = pl.ds(t * TF if isinstance(t, int) else pl.multiple_of(t * TF, TF), TF)
        return pltpu.make_async_copy(xb.at[r], zo.at[r], lsem.at[t])

    with scope('F2a'):
        new[3].mate(4)
        w1c[0].start()
        w2c[0].start()
        w1c[1].start()
        w1c[0].wait()
        step(hj=0)
    with scope('F2b'):
        new[3].fwd_a()
        w1c[2].start()
        w1c[1].wait()
        w2c[0].wait()
        step(hj=1, pj=0)
    def right_in():
        new[3].mate(8)
        new[3].mate(7)
        w2c[1].start()
        w2c[2].start()

    def opposite_in():
        new[3].mate(9)
        w2c[3].start()

    with scope('F2c'):
        new[3].fwd_b()
        w1c[3].start()
        w1c[2].wait()
        step(hj=2, hook=right_in)
    with scope('F2d'):
        w1c[3].wait()
        w2c[1].wait()
        step(hj=3, pj=1, hook=new[3].fin)
    with scope('F2e'):
        w2c[2].wait()
        step(pj=2, hook=opposite_in)
    with scope('F2f'):
        w2c[3].wait()
        step(pj=3, last=True)
    with scope('end'):
        for t in range(T // TF):
            zout(t).wait()
        for key in list(pending):
            sent(key)


def copy_out(*refs):
    m = (len(refs) - 2) // 3
    src, out, bufs, isem, osem = refs[:m], refs[m:2 * m], refs[2 * m:3 * m], refs[-2], refs[-1]
    ins, outs = [], []
    for e in range(m):
        h = src[e].shape[0] // 2
        for p in range(2):
            v = pl.ds(p * h, h)
            ins.append(pltpu.make_async_copy(src[e].at[v], bufs[e].at[v], isem.at[e, p]))
            outs.append(pltpu.make_async_copy(bufs[e].at[v], out[e].at[v], osem.at[e, p]))
    for cp in ins:
        cp.start()
    for a, b in zip(ins, outs):
        a.wait()
        b.start()
    for cp in outs:
        cp.wait()


def solution(mesh):
    n = mesh.shape['fsdp']
    tok4 = P(None, ('mp', 'fsdp'), None, None)
    tok3 = P(('mp', 'fsdp'), None, None)
    rows = P(None, ('mp', 'fsdp'), None)

    def body(x, dy, xn, w1, w2, g1, g2, m1, m2, v1, v2, hp, step):
        nl, b, t, d = x.shape
        T = b * t
        R = w2.shape[1]
        FB = 2 * R
        nc = n // 2
        hbm = pl.BlockSpec(memory_space=pltpu.HBM)
        smem = pl.BlockSpec(memory_space=pltpu.SMEM)
        sd = jax.ShapeDtypeStruct
        state = [sd(w1.shape, F32), sd(w2.shape, F32)] * 3
        res = pl.pallas_call(
            functools.partial(kernel, n),
            out_shape=state + [
                sd((T, d), BF), sd((2 * nl, n, R, d), BF), sd((2 * nl, n, R, d), BF),
                sd((2 * nl, 2, R, d), F32)],
            in_specs=[hbm] * 11 + [smem] * 2,
            out_specs=[hbm] * 10,
            scratch_shapes=[
                pltpu.VMEM((T, d), BF), pltpu.VMEM((d, T), BF),
                pltpu.VMEM((T, d), BF), pltpu.VMEM((d, T), BF),
                pltpu.VMEM((T, FB), BF), pltpu.VMEM((T, FB), BF),
                pltpu.VMEM((max(6 * R, T), d), F32),
                pltpu.VMEM((n, R, d), BF), pltpu.VMEM((n, R, d), BF),
                pltpu.VMEM((2, nc, R, d), BF),
                pltpu.VMEM((2, nc, R, d), F32),
                pltpu.VMEM((2 * nl, R // 2, d), F32), pltpu.VMEM((2 * nl, R // 2, d), F32),
                pltpu.VMEM((2 * nl, R, d), BF),
                pltpu.VMEM((2, n, d // n, FB), BF), pltpu.VMEM((2, 2, R, d), BF),
                pltpu.SemaphoreType.DMA((4 * nl, 10)), pltpu.SemaphoreType.DMA((4 * nl, 10)),
                pltpu.SemaphoreType.DMA((2 * nl, 10)), pltpu.SemaphoreType.DMA((2 * nl, 10)),
                pltpu.SemaphoreType.DMA((2, 2)), pltpu.SemaphoreType.DMA((18,)),
                pltpu.SemaphoreType.DMA((12,)),
            ],
            compiler_params=pltpu.CompilerParams(
                collective_id=0, has_side_effects=True, vmem_limit_bytes=67043328),
        )(x.reshape(nl, T, d), dy.reshape(T, d), xn.reshape(T, d),
          w1, w2, g1, g2, m1, m2, v1, v2, hp, step)
        state = state + [sd((T, d), BF)]
        out = pl.pallas_call(
            copy_out,
            out_shape=state,
            in_specs=[hbm] * 7,
            out_specs=[hbm] * 7,
            scratch_shapes=[pltpu.VMEM(a.shape, a.dtype) for a in state] + [
                pltpu.SemaphoreType.DMA((7, 2)), pltpu.SemaphoreType.DMA((7, 2))],
            compiler_params=pltpu.CompilerParams(vmem_limit_bytes=60 << 20),
        )(*res[:7])
        return tuple(out[:6]) + (out[6].reshape(b, t, d),)

    return jax.shard_map(body, mesh=mesh,
                         in_specs=(tok4, tok3, tok3) + (rows,) * 8 + (P(), P()),
                         out_specs=(rows,) * 6 + (tok3,), check_vma=False)
```

```python
import functools

import jax
import jax.numpy as jnp
from jax import lax
from jax.experimental import pallas as pl
from jax.experimental.pallas import tpu as pltpu
from jax.sharding import PartitionSpec as P

F32 = jnp.float32
BF = jnp.bfloat16
TM = 512
TF = 1024
GC = 0.7978845608028654
GA = 0.044715


def gelu(h):
    return h * (0.5 * (1.0 + jnp.tanh(GC * (h + GA * (h * h * h)))))


def gelu_grad(h):
    s = h * h
    t = jnp.tanh(GC * (h + GA * (s * h)))
    cdf = 0.5 + 0.5 * t
    dt = (0.5 * GC) * (1.0 - t * t) * (1.0 + (3.0 * GA) * s)
    return h * cdf, cdf + h * dt


def dot(a, b):
    return jnp.dot(a, b, preferred_element_type=F32)


def dot_t(a, b):
    return lax.dot_general(a, b, (((1,), (1,)), ((), ())), preferred_element_type=F32)


def offset(j):
    if isinstance(j, int):
        return (2, 1, 3, 0)[j]
    return jnp.where(j == 0, 2, jnp.where(j == 1, 1, jnp.where(j == 2, 3, 0)))


def ipow(b, t):
    r = b * b
    for e in (3, 4, 5):
        r = r * jnp.where(t >= e, b, 1.0)
    return r


def kernel(n, x, dy, xn, w1, w2, g1, g2, m1, m2, v1, v2, hp, step,
           w1n, w2n, m1n, m2n, v1n, v2n, zo, go, gn, rp,
           xb, xt, yb, yt, ab, db, acc, p1, p2, pq, tb, ra, rb, nb, w1s, w2s,
           ag_s, ag_r, rs_s, rs_r, wsem, lsem, osem):
    nl, T, D = x.shape
    R = w2.shape[1]
    FB = 2 * R
    H = R // 2
    nc = n // 2
    D8 = D // n
    nt = T // TM
    me = lax.axis_index('fsdp')
    c = lax.div(me, 2)
    k = lax.rem(me, 2)
    cl, cr, co = lax.rem(c + nc - 1, nc), lax.rem(c + 1, nc), lax.rem(c + 2, nc)
    i, iq = 2 * c + k, 2 * c + 1 - k
    il, ir, io = 2 * cl + k, 2 * cr + k, 2 * co + k
    ilq, irq, ioq = 2 * cl + 1 - k, 2 * cr + 1 - k, 2 * co + 1 - k
    hA, hB = pl.ds(0, H), pl.ds(H, H)
    LEFT, RIGHT, MATE = il, ir, iq

    barrier = pltpu.get_barrier_semaphore()
    for dev in (LEFT, RIGHT, MATE):
        pl.semaphore_signal(barrier, inc=1, device_id={'fsdp': dev})

    def rmake(src, dst, ss, rs, dev):
        return pltpu.make_async_remote_copy(
            src_ref=src[0].at[src[1:]], dst_ref=dst[0].at[dst[1:]], send_sem=ss[0].at[ss[1:]],
            recv_sem=rs[0].at[rs[1:]], device_id={'fsdp': dev})

    def rwait(dst, ss, rs, dev):
        rmake(dst, dst, ss, rs, dev).wait_recv()

    def rsent(src, ss, rs):
        rmake(src, src, ss, rs, MATE).wait_send()

    class Gather:
        def __init__(self, m, G, src):
            self.m, self.G, self.src = m, G, src

        def put(self, t, src, dst, dev):
            rmake(src, dst, (ag_s, self.m), (ag_r, self.m, t), dev).start()

        def got(self, t, dst, dev):
            rwait(dst, (ag_s, self.m), (ag_r, self.m, t), dev)

        def drain(self):
            rsent((self.G, self.m, pl.ds(0, n - 1)), (ag_s, self.m), (ag_r, self.m, 0))

        def start(self):
            self.start_a()
            self.start_b()

        def fwd(self):
            self.fwd_a()
            self.fwd_b()

        def start_a(self):
            G, m, src = self.G, self.m, self.src
            self.put(0, src + (hA,), (G, m, i, hA), RIGHT)
            self.put(3, src + (hB,), (G, m, i, hB), LEFT)
            self.put(4, src, (G, m, i), MATE)

        def start_b(self):
            G, m, src = self.G, self.m, self.src
            self.put(1, src + (hB,), (G, m, i, hB), RIGHT)
            self.put(2, src + (hA,), (G, m, i, hA), LEFT)

        def fwd_a(self):
            G, m = self.G, self.m
            self.got(0, (G, m, il, hA), LEFT)
            self.put(5, (G, m, il, hA), (G, m, il, hA), RIGHT)
            self.got(3, (G, m, ir, hB), RIGHT)
            self.put(6, (G, m, ir, hB), (G, m, ir, hB), LEFT)

        def fwd_b(self):
            G, m = self.G, self.m
            self.got(1, (G, m, il, hB), LEFT)
            self.put(7, (G, m, il), (G, m, il), MATE)
            self.got(2, (G, m, ir, hA), RIGHT)
            self.put(8, (G, m, ir), (G, m, ir), MATE)

        def fin(self):
            G, m = self.G, self.m
            self.got(5, (G, m, io, hA), LEFT)
            self.got(6, (G, m, io, hB), RIGHT)
            self.put(9, (G, m, io), (G, m, io), MATE)

        def mate(self, t):
            G, m = self.G, self.m
            j = {4: iq, 7: ilq, 8: irq, 9: ioq}[t]
            self.got(t, (G, m, j), MATE)

        def full(self):
            for t in (4, 7, 8, 9):
                self.mate(t)

    old = [Gather(m, go, (nb, m)) for m in range(2 * nl)]
    new = [Gather(m, gn, (nb, m)) for m in range(2 * nl)]

    dest = (co, cr, cl, c)
    mine = tuple(2 * d + k for d in dest)
    theirs = tuple(2 * d + 1 - k for d in dest)

    def rset(m):
        return 1 - m % 2

    def part(m):
        return p2 if m % 2 else p1

    def rput(m, p, e, src, dst, dev):
        rmake(src, dst, (rs_s, m, p), (rs_r, m, e), dev).start()

    def rgot(m, e, dst, dev):
        rwait(dst, (rs_s, m, 0), (rs_r, m, e), dev)

    def rs_x0(m, sl):
        rput(m, 0, sl, (part(m), theirs[sl]), (pq, rset(m), sl), MATE)

    def rs_x0_done(m):
        rsent((pq, rset(m)), (rs_s, m, 0), (rs_r, m, 0))

    def rs_pair_done(m):
        rsent((rp, m), (rs_s, m, 1), (rs_r, m, 6))

    def rs_mid_done(m):
        rsent((rp, m, 0), (rs_s, m, 2), (rs_r, m, 6))

    def rs_pair(m, sl):
        s = rset(m)
        if sl == 0 and m + 2 < 2 * nl:
            rs_pair_done(m + 2)
        rgot(m, sl, (pq, s, sl), MATE)
        tb[s, sl] = part(m)[mine[sl]].astype(F32) + pq[s, sl].astype(F32)
        if sl == 0:
            rput(m, 1, 4, (tb, s, 0, hA), (ra, m), LEFT)
            rput(m, 1, 5, (tb, s, 0, hB), (rb, m), RIGHT)
        elif sl == 1:
            rput(m, 1, 6, (tb, s, 1, hA), (rp, m, 0, hA), RIGHT)
        elif sl == 2:
            rput(m, 1, 6, (tb, s, 2, hB), (rp, m, 1, hB), LEFT)

    def rs_mid(m):
        s = rset(m)
        rgot(m, 4, (ra, m), RIGHT)
        ra[m] = ra[m] + tb[s, 2, hA]
        rput(m, 2, 6, (ra, m), (rp, m, 1, hA), LEFT)
        rgot(m, 5, (rb, m), LEFT)
        rb[m] = rb[m] + tb[s, 1, hB]
        rput(m, 2, 6, (rb, m), (rp, m, 0, hB), RIGHT)

    def pieces(m, arr, row):
        l = m // 2
        if m % 2:
            return [(arr.at[l], acc.at[pl.ds(row, R)])]
        return [(arr.at[l, :, pl.ds(q * FB, FB)], acc.at[pl.ds(row + q * D8, D8)]) for q in range(nc)]

    ins = {0: (w1, g1, m1, v1), 1: (w2, g2, m2, v2)}
    outs = {0: (w1n, m1n, v1n), 1: (w2n, m2n, v2n)}

    def adam_copies(m):
        cps = []
        for j, arr in enumerate(ins[m % 2]):
            for hbm, vm in pieces(m, arr, j * R):
                cps.append(pltpu.make_async_copy(hbm, vm, lsem.at[j]))
        return cps

    def adam_load(m):
        for cp in adam_copies(m):
            cp.start()

    def arrived(row, rows, sem):
        pltpu.make_async_copy(acc.at[pl.ds(row, rows)], acc.at[pl.ds(row, rows)], sem).wait()

    def adam_run(m):
        s = rset(m)
        rgot(m, 6, (rp, m), LEFT)
        for e in range(2):
            pltpu.make_async_copy(rp.at[m, e], acc.at[pl.ds((4 + e) * R, R)], lsem.at[4]).start()
        for j in range(4):
            arrived(j * R, R, lsem.at[j])
        arrived(4 * R, 2 * R, lsem.at[4])
        old[m].drain()
        lr, b1, b2, eps, wd = [hp[j] for j in range(5)]
        c1 = 1.0 - ipow(b1, step[0])
        c2 = 1.0 - ipow(b2, step[0])
        ch = 32

        @pl.loop(0, R // ch)
        def _(e):
            o = pl.multiple_of(e * ch, ch)
            rows = [pl.ds(j * R + o, ch) for j in range(6)]
            S = tb[s, 3, pl.ds(o, ch)] + acc[rows[4]] + acc[rows[5]]
            w = acc[rows[0]]
            g = (acc[rows[1]] + S) * 0.5
            mn = b1 * acc[rows[2]] + (1.0 - b1) * g
            vn = b2 * acc[rows[3]] + (1.0 - b2) * g * g
            upd = (mn / c1) / (jnp.sqrt(vn / c2) + eps)
            wn = w - lr * (upd + wd * w)
            acc[rows[0]] = wn
            acc[rows[2]] = mn
            acc[rows[3]] = vn
            nb[m, pl.ds(o, ch)] = wn.astype(BF)

        for e, (arr, j) in enumerate(zip(outs[m % 2], (0, 2, 3))):
            for hbm, vm in pieces(m, arr, j * R):
                pltpu.make_async_copy(vm, hbm, osem.at[e]).start()

    def adam_done(m):
        for e, j in enumerate((0, 2, 3)):
            arrived(j * R, R, osem.at[e])

    def wcopy(G, l, q, slot, kind):
        if kind:
            return pltpu.make_async_copy(G.at[2 * l + 1, pl.ds(2 * q, 2)], w2s.at[slot], wsem.at[slot, 1])
        return pltpu.make_async_copy(G.at[2 * l, :, pl.ds(q * D8, D8)], w1s.at[slot], wsem.at[slot, 0])

    def wcopies(*a):
        return wcopy(*a, 0), wcopy(*a, 1)

    def wload(*a):
        for cp in wcopies(*a):
            cp.start()

    def wwait(*a):
        for cp in wcopies(*a):
            cp.wait()

    def tile(t):
        return pl.ds(pl.multiple_of(t * TM, TM), TM)

    def w1v(slot):
        return w1s[slot].reshape(D, FB)

    def w2v(slot):
        return w2s[slot].reshape(FB, D)

    def bwd_fused(slot):
        @pl.loop(0, nt)
        def _(t):
            r = tile(t)
            h = dot(xb[r, :], w1v(slot))
            da = dot_t(yb[r, :], w2v(slot))
            a, gp = gelu_grad(h)
            ab[r, :] = a.astype(BF)
            db[r, :] = (da * gp).astype(BF)

    def bwd_p2(q):
        @pl.loop(0, D // 256)
        def _(t):
            o = pl.ds(pl.multiple_of(t * 256, 256), 256)
            r = dot(yt[o, :], ab[...])
            p2[pl.ds(2 * q, 2), :, o] = r.T.astype(BF).reshape(2, R, 256)

    def bwd_p1(q):
        @pl.loop(0, 2)
        def _(t):
            o = pl.ds(pl.multiple_of(t * (D // 2), D // 2), D // 2)
            r = dot(xt[o, :], db[...])
            p1[pl.ds(t * (n // 2), n // 2), pl.ds(pl.multiple_of(q * D8, D8), D8), :] = (
                r.astype(BF).reshape(n // 2, D8, FB))

    def bwd_dx(slot, first):
        @pl.loop(0, nt)
        def _(t):
            r = tile(t)
            z = dot_t(db[r, :], w1v(slot))
            acc[r, :] = jnp.where(first, yb[r, :].astype(F32), acc[r, :]) + z

    def transpose(dst, src):
        @pl.loop(0, T // 256)
        def _(t):
            o = pl.ds(pl.multiple_of(t * 256, 256), 256)
            dst[:, o] = src[o, :].T

    order = (c, cr, cl, co)
    abuf = (ab, db, yb, xb)

    def hidden(l, hooks):
        cps = [wcopy(gn, l, order[j], j % 2, 0) for j in range(nc)]
        cps[0].start()
        for j in range(nc):
            if j + 1 < nc:
                cps[j + 1].start()
            cps[j].wait()

            @pl.loop(0, nt)
            def _(t):
                r = tile(t)
                xv = xb[r, :]
                if j == 0:
                    acc[r, :] = xv.astype(F32)
                abuf[j][r, :] = gelu(dot(xv, w1v(j % 2))).astype(BF)
            if j in hooks:
                with jax.named_scope(f'hookH{j}'):
                    hooks[j]()

    def project(l, ready, hooks, done, late):
        cps = [wcopy(gn, l, order[j], j % 2, 1) for j in range(nc)]
        ready(0)
        cps[0].start()
        for j in range(nc):
            if j + 1 < late:
                with jax.named_scope(f'ready{j + 1}'):
                    ready(j + 1)
                cps[j + 1].start()
            elif j >= late:
                with jax.named_scope(f'ready{j}'):
                    ready(j)
                cps[j].start()
            cps[j].wait()

            @pl.loop(0, nt)
            def _(t):
                r = tile(t)
                z = acc[r, :] + dot(abuf[j][r, :], w2v(j % 2))
                if j == nc - 1:
                    xb[r, :] = z.astype(BF)
                    done(t)
                else:
                    acc[r, :] = z
            if j in hooks:
                with jax.named_scope(f'hookP{j}'):
                    hooks[j]()

    def narrow(dst):
        @pl.loop(0, nt)
        def _(t):
            r = tile(t)
            dst[r, :] = acc[r, :].astype(BF)

    def at(j, hooks):
        for jj, fn in hooks.items():
            @pl.when(j == jj)
            def _():
                fn()

    def blocks(G, l, off, count, stages, ready=None):
        wload(G, l, lax.rem(c + off(0), nc), 0)

        @pl.loop(0, count)
        def _(j):
            s = lax.rem(j, 2)
            q = lax.rem(c + off(j), nc)

            @pl.when(j + 1 < count)
            def _():
                wload(G, l, lax.rem(c + off(j + 1), nc), 1 - s)
            wwait(G, l, q, s)
            for name, fn, hooks in stages:
                with jax.named_scope(name):
                    fn(j, q, s)
                with jax.named_scope(name + 'Hook'):
                    at(j, hooks)

    scope = jax.named_scope

    with scope('start'):
        w_in = [[pltpu.make_async_copy(a, b, lsem.at[m]) for a, b in pieces(m, ins[m % 2][0], m * R)]
                for m in range(2 * nl)]
        for m in (2, 3, 0, 1):
            for cp in w_in[m]:
                cp.start()
        tok_in = [pltpu.make_async_copy(x.at[1], xb, wsem.at[0, 0]),
                  pltpu.make_async_copy(dy, yb, wsem.at[0, 1])]
        for cp in tok_in:
            cp.start()
        own_out = [pltpu.make_async_copy(nb.at[m], go.at[m, i], osem.at[m]) for m in range(2 * nl)]
        for m in (2, 3, 0, 1):
            arrived(m * R, R, lsem.at[m])
            nb[m] = acc[pl.ds(m * R, R), :].astype(BF)
            if m == 2:
                pl.semaphore_wait(barrier, 3)
            if m >= 2:
                old[m].start()
            own_out[m].start()
        for cp in tok_in:
            cp.wait()
    with scope('f2'):
        old[2].fwd()
    with scope('xt'):
        transpose(xt, xb)
        for cp in own_out:
            cp.wait()
    with scope('f3'):
        old[3].fwd()
        old[0].start()
        old[1].start()
    with scope('yt'):
        transpose(yt, yb)
    with scope('full23'):
        old[2].fin()
        old[2].full()
        old[3].fin()
        old[3].full()

    def c2_2():
        old[0].fin()
        rs_pair(3, 2)

    def c2_3():
        old[1].fin()
        for sl in range(4):
            rs_x0(2, sl)
        rs_pair(3, 3)

    blocks(go, 1, offset, nc, [
        ('A2', lambda j, q, s: bwd_fused(s), {2: lambda: rs_pair(3, 1), 3: lambda: rs_mid(3)}),
        ('B2', lambda j, q, s: bwd_p2(q), {
            0: lambda: rs_x0(3, 0),
            1: lambda: (rs_x0(3, 1), rs_pair(3, 0)),
            2: lambda: rs_x0(3, 2),
            3: lambda: rs_x0(3, 3)}),
        ('C2', lambda j, q, s: bwd_p1(q), {
            0: old[0].fwd, 1: old[1].fwd, 2: c2_2, 3: c2_3}),
        ('D2', lambda j, q, s: bwd_dx(s, j == 0), {}),
    ])
    with scope('mid2'):
        xin = pltpu.make_async_copy(x.at[0], xb, lsem.at[5])
        xin.start()
        rs_x0_done(3)
        for sl in range(4):
            rs_pair(2, sl)
        rs_x0_done(2)
    with scope('tr2'):
        narrow(yb)
        transpose(yt, yb)
        xin.wait()
        transpose(xt, xb)
    with scope('full01'):
        old[0].full()
        old[1].full()

    adam_load(3)

    def up3():
        rs_pair(1, 0)
        adam_run(3)

    def up2():
        adam_done(3)
        adam_load(2)

    def up1():
        rs_pair(1, 2)
        adam_run(2)

    blocks(go, 0, offset, nc, [
        ('A1', lambda j, q, s: bwd_fused(s), {
            1: lambda: rs_mid(2), 2: lambda: rs_pair(1, 1), 3: up1}),
        ('B1', lambda j, q, s: bwd_p2(q), {jj: functools.partial(rs_x0, 1, jj) for jj in range(nc)}),
        ('C1', lambda j, q, s: bwd_p1(q), {1: up3, 2: up2}),
    ])
    with scope('mid1'):
        for sl in range(4):
            rs_x0(0, sl)
        xin = pltpu.make_async_copy(xn, xb, wsem.at[0, 0])
        xin.start()
        adam_done(2)
        adam_load(1)
        rs_mid(1)
        rs_pair(1, 3)
        for sl in range(4):
            rs_pair(0, sl)
    with scope('adam1'):
        adam_run(1)
        adam_done(1)
        adam_load(0)
    with scope('mid0'):
        rs_mid(0)
        new[1].start_a()
    own_out = [pltpu.make_async_copy(nb.at[m], gn.at[m, i], wsem.at[m // 2, m % 2]) for m in range(2 * nl)]
    with scope('adam0'):
        xin.wait()
        adam_run(0)
        new[0].start()
        for cp in own_out:
            cp.start()
    with scope('fn0'):
        new[0].fwd_a()
        new[1].start_b()
        new[1].fwd_a()
        new[0].fwd_b()
        for cp in own_out:
            cp.wait()
        adam_done(0)
    with scope('full_n0'):
        new[0].fin()
        new[2].start()
        new[0].full()

    def nx2():
        new[2].fwd_a()
        new[3].start()

    with scope('H1'):
        hidden(0, {1: new[1].fwd_b, 3: new[1].fin})
    with scope('P1'):
        project(0, lambda j: new[1].mate((4, 8, 7, 9)[j]), {0: nx2, 2: new[2].fwd_b}, lambda t: None, nc)
    with scope('full_n2'):
        new[2].fin()
        new[2].full()

    w1c = [wcopy(gn, 1, order[j], j % 2, 0) for j in range(nc)]
    w2c = [wcopy(gn, 1, order[j], j % 2, 1) for j in range(nc)]

    def step(hj=None, pj=None, last=False, hook=None):
        @pl.loop(0, T // TF)
        def _(t):
            r = pl.ds(pl.multiple_of(t * TF, TF), TF)
            if hook is not None:
                @pl.when(t == T // TF - 1)
                def _():
                    hook()
            if pj is not None:
                z = acc[r, :] + dot(abuf[pj][r, :], w2v(pj % 2))
            if hj is not None:
                xv = xb[r, :]
                if hj == 0:
                    acc[r, :] = xv.astype(F32)
                abuf[hj][r, :] = gelu(dot(xv, w1v(hj % 2))).astype(BF)
            if last:
                xb[r, :] = z.astype(BF)
                zout(t).start()
            elif pj is not None:
                acc[r, :] = z

    def zout(t):
        r = pl.ds(t * TF if isinstance(t, int) else pl.multiple_of(t * TF, TF), TF)
        return pltpu.make_async_copy(xb.at[r], zo.at[r], lsem.at[t])

    def right_in():
        new[3].mate(8)
        new[3].mate(7)
        w2c[1].start()
        w2c[2].start()

    def opposite_in():
        new[3].mate(9)
        w2c[3].start()

    with scope('F2H0'):
        new[3].mate(4)
        w1c[0].start()
        w2c[0].start()
        w1c[1].start()
        w1c[0].wait()
        step(hj=0)
    with scope('F2P0'):
        w2c[0].wait()
        w1c[2].start()
        step(pj=0, hook=new[3].fwd_a)
    with scope('F2H1'):
        w1c[1].wait()
        step(hj=1)
    with scope('F2H2'):
        w1c[3].start()
        w1c[2].wait()
        step(hj=2, hook=new[3].fwd_b)
    with scope('F2H3'):
        w1c[3].wait()
        step(hj=3, hook=right_in)
    with scope('F2P1'):
        w2c[1].wait()
        step(pj=1, hook=new[3].fin)
    with scope('F2P2'):
        w2c[2].wait()
        step(pj=2, hook=opposite_in)
    with scope('F2P3'):
        w2c[3].wait()
        step(pj=3, last=True)
    with scope('end'):
        for t in range(T // TF):
            zout(t).wait()
        for m in range(2 * nl):
            new[m].drain()
            rs_mid_done(m)
        for m in range(2):
            rs_x0_done(m)
            rs_pair_done(m)


def copy_out(*refs):
    m = (len(refs) - 2) // 3
    src, out, bufs, isem, osem = refs[:m], refs[m:2 * m], refs[2 * m:3 * m], refs[-2], refs[-1]
    ins, outs = [], []
    for e in range(m):
        h = src[e].shape[0] // 2
        for p in range(2):
            v = pl.ds(p * h, h)
            ins.append(pltpu.make_async_copy(src[e].at[v], bufs[e].at[v], isem.at[e, p]))
            outs.append(pltpu.make_async_copy(bufs[e].at[v], out[e].at[v], osem.at[e, p]))
    for cp in ins:
        cp.start()
    for a, b in zip(ins, outs):
        a.wait()
        b.start()
    for cp in outs:
        cp.wait()


def solution(mesh):
    n = mesh.shape['fsdp']
    tok4 = P(None, ('mp', 'fsdp'), None, None)
    tok3 = P(('mp', 'fsdp'), None, None)
    rows = P(None, ('mp', 'fsdp'), None)

    def body(x, dy, xn, w1, w2, g1, g2, m1, m2, v1, v2, hp, step):
        nl, b, t, d = x.shape
        T = b * t
        R = w2.shape[1]
        FB = 2 * R
        nc = n // 2
        hbm = pl.BlockSpec(memory_space=pltpu.HBM)
        smem = pl.BlockSpec(memory_space=pltpu.SMEM)
        sd = jax.ShapeDtypeStruct
        state = [sd(w1.shape, F32), sd(w2.shape, F32)] * 3
        res = pl.pallas_call(
            functools.partial(kernel, n),
            out_shape=state + [
                sd((T, d), BF), sd((2 * nl, n, R, d), BF), sd((2 * nl, n, R, d), BF),
                sd((2 * nl, 2, R, d), F32)],
            in_specs=[hbm] * 11 + [smem] * 2,
            out_specs=[hbm] * 10,
            scratch_shapes=[
                pltpu.VMEM((T, d), BF), pltpu.VMEM((d, T), BF),
                pltpu.VMEM((T, d), BF), pltpu.VMEM((d, T), BF),
                pltpu.VMEM((T, FB), BF), pltpu.VMEM((T, FB), BF),
                pltpu.VMEM((max(6 * R, T), d), F32),
                pltpu.VMEM((n, R, d), BF), pltpu.VMEM((n, R, d), BF),
                pltpu.VMEM((2, nc, R, d), BF),
                pltpu.VMEM((2, nc, R, d), F32),
                pltpu.VMEM((2 * nl, R // 2, d), F32), pltpu.VMEM((2 * nl, R // 2, d), F32),
                pltpu.VMEM((2 * nl, R, d), BF),
                pltpu.VMEM((2, n, d // n, FB), BF), pltpu.VMEM((2, 2, R, d), BF),
                pltpu.SemaphoreType.DMA((2 * nl,)), pltpu.SemaphoreType.DMA((2 * nl, 10)),
                pltpu.SemaphoreType.DMA((2 * nl, 3)), pltpu.SemaphoreType.DMA((2 * nl, 7)),
                pltpu.SemaphoreType.DMA((2, 2)), pltpu.SemaphoreType.DMA((6,)),
                pltpu.SemaphoreType.DMA((4,)),
            ],
            compiler_params=pltpu.CompilerParams(
                collective_id=0, has_side_effects=True, vmem_limit_bytes=67043328),
        )(x.reshape(nl, T, d), dy.reshape(T, d), xn.reshape(T, d),
          w1, w2, g1, g2, m1, m2, v1, v2, hp, step)
        state = state + [sd((T, d), BF)]
        out = pl.pallas_call(
            copy_out,
            out_shape=state,
            in_specs=[hbm] * 7,
            out_specs=[hbm] * 7,
            scratch_shapes=[pltpu.VMEM(a.shape, a.dtype) for a in state] + [
                pltpu.SemaphoreType.DMA((7, 2)), pltpu.SemaphoreType.DMA((7, 2))],
            compiler_params=pltpu.CompilerParams(vmem_limit_bytes=60 << 20),
        )(*res[:7])
        return tuple(out[:6]) + (out[6].reshape(b, t, d),)

    return jax.shard_map(body, mesh=mesh,
                         in_specs=(tok4, tok3, tok3) + (rows,) * 8 + (P(), P()),
                         out_specs=(rows,) * 6 + (tok3,), check_vma=False)
```
